32 devices in a mesh: ep: 16 (over z, y, x), dp: 2 (over core).
Axes of the slice: x: 2, y: 2, z: 4, core: 2. Of those that a mesh axis runs over, the one named last changes fastest.
Arguments:
- tokens: bfloat16 [2048, 2048], P(('dp', 'ep')), parts along dimension 0, may hold values from -6 to 6
- expert_ids: int32 [2048, 8], P(('dp', 'ep')), parts along dimension 0, may hold values from 0 to 15, all different within a row; in each aligned block of 64 rows (0 to 63, 64 to 127, ...) at most 64 rows name the same one
- gate_probs: float32 [2048, 8], P(('dp', 'ep')), parts along dimension 0, may hold values from 0.05 to 1
- w_gate: bfloat16 [16, 2048, 768], P('ep'), may hold values from -0.125 to 0.125
- w_up: bfloat16 [16, 2048, 768], P('ep'), may hold values from -0.125 to 0.125
- w_down: bfloat16 [16, 768, 2048], P('ep'), may hold values from -0.21875 to 0.21875
Outputs:
- combined: bfloat16 [2048, 2048], P(('dp', 'ep')), parts along dimension 0
The draws below stay inside these ranges and needn't reach their ends.
There are 2 independent parts, one for each index of `dp`. The reference program is written for one: setup_inputs(seed, part) draws one part's arguments, and reference() takes and returns one part's arrays. A program takes and returns all parts, laid end to end along the dimension named above; an argument that names none is the same for every part. Nothing has to cross between parts.
Inputs may be any that keep to these rules, and one draw needn't show every extreme that they name: `expert_ids`: each row names 8 different experts. Among the rows of one index of ep (aligned blocks of 64 rows) no expert is named by more than 64 rows, and in every draw some expert is named by exactly 64 rows of some block. Expert popularity is skewed.
All inputs are finite; a program needn't handle non-finite values.
Results may differ from the reference program's by a relative error of at most 0.0085.
Values may be sent and summed in bfloat16 or wider, within the bound.
A program may use at most 64 MiB of HBM per device.

```python
import math
import jax
import jax.numpy as jnp
import numpy as np
from jax import lax

D = 2048
FF = 768
TOP = 8
TOK_DEV = 64
EXPERTS = 16
TOKENS = 1024
MOST = 64
N_EP = 16


def levels(key, extent, cuts, least, top_value):
    factor_of, own = 1.0, jax.random.fold_in(key, 6)
    for dim, blocks in cuts:
        steps = jnp.exp(jax.random.uniform(jax.random.fold_in(own, dim), (blocks,), jnp.float32, least / len(cuts), top_value / len(cuts)))
        factor_of = factor_of * jnp.repeat(steps, extent[dim] // blocks).reshape([-1 if axis == dim else 1 for axis in range(len(extent))])
    return factor_of


def deal_out(own_key, own, number, rows, count, top, reach, lean):
    sequence = jax.random.permutation(own_key, count)
    crowded, usual = shares(count, rows * top, reach, lean, True), shares(count, rows * top, reach, lean, False)
    places = jnp.arange(count)

    def named(lengths, offset_by):
        used = int((lengths > 0).sum())
        fixed = max(1, used // 4)
        passed = fixed + (places - fixed + offset_by * (used - fixed)) % max(1, count - fixed)
        return jnp.zeros((count,), jnp.int32).at[sequence[jnp.where(places < fixed, places, passed)]].set(jnp.asarray(lengths, jnp.int32))

    lengths = jnp.where(number % 4 == 0, named(crowded, number // 4), named(usual, number - number // 4 - 1))
    mixed = jax.random.permutation(jax.random.fold_in(own, 3), count)
    source_of, receiver = mixed[0:count // 2 * 2:2], mixed[1:count // 2 * 2:2]
    margin = jnp.minimum(lengths[source_of] - 1, reach - lengths[receiver]) // 2
    margin = jnp.where((source_of == sequence[0]) | (receiver == sequence[0]) | (lengths[receiver] == 0), 0, jnp.maximum(margin, 0))
    passed = jax.random.randint(jax.random.fold_in(own, 4), (count // 2,), 0, 1 << 20) % (margin + 1)
    lengths = lengths.at[source_of].add(-passed).at[receiver].add(passed)
    labels = jnp.searchsorted(jnp.cumsum(lengths), jnp.arange(rows * top), side="right").astype(jnp.int32)
    grid = labels.reshape(top, rows).T
    grid = grid[jax.random.permutation(jax.random.fold_in(own, 1), rows)]
    offset_by = jax.random.randint(jax.random.fold_in(own, 2), (rows, 1), 0, top)
    return jnp.take_along_axis(grid, (jnp.arange(top)[None, :] + offset_by) % top, axis=1)


def shares(amount, total, limit, skew, full):
    loads = [(1 << 20) // math.isqrt(standing ** skew) + 1 for standing in range(1, amount + 1)]
    largest = limit if full else min(limit, max(-(-total // amount), total * loads[0] // sum(loads)))
    least = 1 if total - largest >= amount - 1 else 0
    given, rest = [largest] + [least] * (amount - 1), total - largest - least * (amount - 1)
    while rest > 0:
        movable = [i for i in range(1, amount) if given[i] < largest] or [i for i in range(1, amount) if given[i] < limit]
        mass, left = sum([loads[i] for i in movable]), rest
        for i in movable:
            extra = min(limit - given[i], max(1, left * loads[i] // mass), rest)
            given[i] = given[i] + extra
            rest = rest - extra
    return np.array(given)


def gaussian(own_key, shape, deviation, limit, cuts=(), kind=jnp.bfloat16):
    level = levels(own_key, shape, cuts, -0.22, 0.18) if cuts else 1.0
    values = jax.random.normal(own_key, shape, jnp.float32) * deviation * level
    return jnp.minimum(jnp.maximum(values, -limit), limit).astype(kind)


def setup_inputs(seed: int = 0, part: int = 0) -> dict:
    arg_keys = jax.random.split(jax.random.key(seed), 7)
    part_keys = jax.random.split(jax.random.fold_in(arg_keys[6], part), 7)
    tokens = gaussian(part_keys[0], (TOKENS, D), 1.0, 6.0, ((0, 16),))
    expert_ids_keys = jax.random.split(jax.random.fold_in(part_keys[1], 1), TOKENS // TOK_DEV)
    expert_ids_turns = jax.random.permutation(jax.random.fold_in(part_keys[1], 3), TOKENS // TOK_DEV)
    expert_ids = jax.vmap(lambda own, number: deal_out(jax.random.fold_in(part_keys[1], 2), own, number, TOK_DEV, EXPERTS, TOP, MOST, 2))(expert_ids_keys, expert_ids_turns).reshape((TOKENS, TOP))
    gate_probs = jnp.clip(0.05 + 0.95 * jax.random.uniform(part_keys[2], (TOKENS, TOP), jnp.float32) ** levels(part_keys[2], (TOKENS, TOP), ((0, 16),), -0.2, 0.2), 0.05, 1.0)
    w_gate = gaussian(arg_keys[3], (EXPERTS, D, FF), D ** -0.5, 0.125, ((0, 16),))
    w_up = gaussian(arg_keys[4], (EXPERTS, D, FF), D ** -0.5, 0.125, ((0, 16),))
    w_down = gaussian(arg_keys[5], (EXPERTS, FF, D), FF ** -0.5, 0.21875, ((0, 16),))
    return dict(tokens=tokens, expert_ids=expert_ids, gate_probs=gate_probs, w_gate=w_gate, w_up=w_up, w_down=w_down)


def expert_ffn(row_block, gate_matrix, up_matrix, down_matrix):
    gate_act = jnp.dot(row_block, gate_matrix, preferred_element_type=jnp.float32)
    up_act = jnp.dot(row_block, up_matrix, preferred_element_type=jnp.float32)
    hidden = (jax.nn.silu(gate_act) * up_act).astype(jnp.bfloat16)
    return jnp.dot(hidden, down_matrix, preferred_element_type=jnp.float32).astype(jnp.bfloat16)


def reference(tokens, expert_ids, gate_probs, w_gate, w_up, w_down):
    experts = w_gate.shape[0]
    capacity = N_EP * MOST
    flat_ids = expert_ids.reshape(-1).astype(jnp.int32)
    owners = (jnp.arange(flat_ids.shape[0], dtype=jnp.int32) // TOP).astype(jnp.int32)
    onehot = (flat_ids[:, None] == jnp.arange(experts, dtype=jnp.int32)[None, :]).astype(jnp.int32)
    within_rank = jnp.sum((jnp.cumsum(onehot, axis=0) - onehot) * onehot, axis=1).astype(jnp.int32)
    slot_index = (flat_ids * capacity + within_rank).astype(jnp.int32)
    slot_token = jnp.zeros((experts * capacity,), jnp.int32).at[slot_index].set(owners)
    filled = jnp.zeros((experts * capacity,), jnp.bool_).at[slot_index].set(True)

    def per_expert(expert_index):
        row_start = (expert_index * capacity).astype(jnp.int32)
        chosen = lax.dynamic_slice_in_dim(slot_token, row_start, capacity, 0)
        present = lax.dynamic_slice_in_dim(filled, row_start, capacity, 0)
        row_block = jnp.where(present[:, None], tokens[chosen], jnp.zeros((), jnp.bfloat16))
        return expert_ffn(row_block, w_gate[expert_index], w_up[expert_index], w_down[expert_index])

    outputs = lax.map(per_expert, jnp.arange(experts, dtype=jnp.int32))
    picked = outputs.reshape(-1, tokens.shape[1])[slot_index].astype(jnp.float32)
    picked = picked.reshape(tokens.shape[0], TOP, tokens.shape[1])
    weights = gate_probs / jnp.sum(gate_probs, axis=1, keepdims=True)
    combined = jnp.sum(picked * weights[:, :, None], axis=1)
    return combined.astype(jnp.bfloat16)
```

```python
import functools

import jax
import jax.numpy as jnp
from jax import lax
from jax.experimental import pallas as pl
from jax.experimental.pallas import tpu as pltpu
from jax.sharding import PartitionSpec as P

LANES = 128
ROWS = 16
TILE = 256


def kernel(n, cfg, tokens, ids, probs, wg_hbm, wu_hbm, wd_hbm, out,
           x_buf, y_buf, r1, r2, r3, gates, hidden, wg, wu, wd,
           ag1_s, ag1_r, agz_s, agz_r, ag3_s, ag3_r,
           rs1_s, rs1_r, rs2_s, rs2_r, rs3_s, rs3_r, loc):
    nz = n // 4
    toks, width = out.shape
    chunks = toks // ROWS
    half = width // 2
    ff = wg.shape[1]
    me = lax.axis_index("ep")
    x, y, z = me % 2, (me // 2) % 2, me // 4
    up, down = z < nz - 1, z > 0
    dev = lambda zz, yy, xx: {"ep": (zz * 2 + yy) * 2 + xx}
    x_nbr, y_nbr = dev(z, y, 1 - x), dev(z, 1 - y, x)
    up_nbr, down_nbr = dev(jnp.minimum(z + 1, nz - 1), y, x), dev(jnp.maximum(z - 1, 0), y, x)

    wcopies = [pltpu.make_async_copy(a, b, loc.at[chunks + i])
               for i, (a, b) in enumerate(((wg_hbm.at[0], wg), (wu_hbm.at[0], wu), (wd_hbm.at[0], wd)))]
    own = []
    for c in range(chunks):
        cp = pltpu.make_async_copy(tokens.at[c * ROWS:(c + 1) * ROWS],
                                   x_buf.at[c, z, y, x, :, 0:width], loc.at[c])
        cp.start()
        own.append(cp)
    for cp in wcopies:
        cp.start()

    barrier = pltpu.get_barrier_semaphore()
    for nbr in (x_nbr, y_nbr):
        pl.semaphore_signal(barrier, inc=1, device_id=nbr, device_id_type=pl.DeviceIdType.MESH)
    for ok, nbr in ((up, up_nbr), (down, down_nbr)):
        @pl.when(ok)
        def _(nbr=nbr):
            pl.semaphore_signal(barrier, inc=1, device_id=nbr, device_id_type=pl.DeviceIdType.MESH)

    p = probs[...]
    w = p / jnp.sum(p, axis=1, keepdims=True)
    lane = lax.broadcasted_iota(jnp.int32, (toks, LANES), 1)
    named = jnp.where(lane < n, lane, lane - n)
    g = jnp.zeros((toks, LANES), jnp.float32)
    for k in range(ids.shape[1]):
        g = g + jnp.where(ids[:, k:k + 1] == named, w[:, k:k + 1], 0.0)
    hi = g.astype(jnp.bfloat16).astype(jnp.float32)
    gates[...] = jnp.where(lane < n, hi, g - hi).astype(jnp.bfloat16)
    gcopies = []
    for c in range(chunks):
        cp = pltpu.make_async_copy(gates.at[c * ROWS:(c + 1) * ROWS],
                                   x_buf.at[c, z, y, x, :, width:width + LANES], loc.at[chunks + 3 + c])
        cp.start()
        gcopies.append(cp)

    pl.semaphore_wait(barrier, 2 + up.astype(jnp.int32) + down.astype(jnp.int32))

    sends = []

    def send(src, dst, ssem, rsem, nbr, ok=None):
        cp = pltpu.make_async_remote_copy(src_ref=src, dst_ref=dst, send_sem=ssem, recv_sem=rsem,
                                          device_id=nbr, device_id_type=pl.DeviceIdType.MESH)
        if ok is None:
            cp.start()
        else:
            pl.when(ok)(cp.start)
        sends.append((cp, ok))

    def landed(dst, rsem):
        pltpu.make_async_copy(dst, dst, rsem).wait()

    cols = (slice(0, half), slice(half, width + LANES))
    ycols = (slice(0, half), slice(half, width))
    first_nbr, last_nbr = (x_nbr, y_nbr), (y_nbr, x_nbr)

    def group(buf, c, h, zz, cs, other=False):
        if h == 0:
            return buf.at[c, zz, (1 - y) if other else y, :, :, cs[0]]
        return buf.at[c, zz, :, (1 - x) if other else x, :, cs[1]]

    def ag_first(c):
        own[c].wait()
        gcopies[c].wait()
        for h in range(2):
            blk = x_buf.at[c, z, y, x, :, cols[h]]
            send(blk, blk, ag1_s.at[c, h], ag1_r.at[c, h], first_nbr[h])

    def ag_last(c, h, zz, ok=None):
        blk = group(x_buf, c, h, zz, cols)
        send(blk, blk, ag3_s.at[c, h, zz], ag3_r.at[c, h, zz], last_nbr[h], ok)

    def ag_step(c, d):
        for h in range(2):
            if d == 0:
                mate = (x_buf.at[c, z, y, 1 - x, :, cols[0]], x_buf.at[c, z, 1 - y, x, :, cols[1]])[h]
                landed(mate, ag1_r.at[c, h])
                blk = group(x_buf, c, h, z, cols)
                send(blk, blk, agz_s.at[c, h, 0, z], agz_r.at[c, h, z], up_nbr, up)
                send(blk, blk, agz_s.at[c, h, 1, z], agz_r.at[c, h, z], down_nbr, down)
                ag_last(c, h, z)
            else:
                for way, origin, ok, more, nbr in ((0, z - d, z - d >= 0, up, up_nbr),
                                                   (1, z + d, z + d <= nz - 1, down, down_nbr)):
                    at = jnp.clip(origin, 0, nz - 1)
                    blk = group(x_buf, c, h, at, cols)
                    pl.when(ok)(functools.partial(landed, blk, agz_r.at[c, h, at]))
                    if d < nz - 1:
                        send(blk, blk, agz_s.at[c, h, way, at], agz_r.at[c, h, at], nbr, jnp.logical_and(ok, more))
                    ag_last(c, h, at, ok)

    def ag_end(c):
        for h in range(2):
            for zz in range(nz):
                landed(group(x_buf, c, h, zz, cols, True), ag3_r.at[c, h, zz])

    rows = n * ROWS

    def ffn_in(c):
        if c == 0:
            wcopies[0].wait()
            wcopies[1].wait()
        tail = x_buf[c, :, :, :, :, width:width + LANES].reshape(rows, LANES).astype(jnp.float32)
        lanes = lax.broadcasted_iota(jnp.int32, (rows, LANES), 1)
        mine = jnp.logical_or(lanes == me, lanes == me + n)
        gcol = jnp.sum(jnp.where(mine, tail, 0.0), axis=1, keepdims=True)

        def body(j, carry):
            at = pl.ds(pl.multiple_of(j * TILE, TILE), TILE)
            xs = x_buf[c, :, :, :, :, 0:width].reshape(rows, width)
            ga = jnp.dot(xs, wg[:, at], preferred_element_type=jnp.float32)
            ua = jnp.dot(xs, wu[:, at], preferred_element_type=jnp.float32)
            hidden[:, at] = (ga / (1.0 + jnp.exp(-ga)) * ua * gcol).astype(jnp.bfloat16)
            return carry

        lax.fori_loop(0, ff // TILE, body, 0)

    def ffn_out(c, part, parts):
        if c == 0 and part == 0:
            wcopies[2].wait()
        per = width // TILE // parts

        def body(j, carry):
            at = pl.ds(pl.multiple_of(j * TILE, TILE), TILE)
            o = jnp.dot(hidden[...], wd[:, at], preferred_element_type=jnp.float32)
            y_buf[c, :, :, :, :, at] = o.astype(jnp.bfloat16).reshape(nz, 2, 2, ROWS, TILE)
            return carry

        lax.fori_loop(part * per, (part + 1) * per, body, 0)

    def rs_first(c, h):
        for i in range(nz):
            zz = jnp.where(z >= nz // 2, i, nz - 1 - i)
            send(group(y_buf, c, h, zz, ycols, True), r1.at[c, h, zz], rs1_s.at[c, h, zz],
                 rs1_r.at[c, h, zz], last_nbr[h])

    def add(c, h, zz, bufs):
        mine = group(y_buf, c, h, zz, ycols)
        total = mine[...].astype(jnp.float32)
        for b in bufs:
            total = total + b[...].astype(jnp.float32)
        mine[...] = total.astype(jnp.bfloat16)

    def rs_step(c, s):
        k = nz - 1 - s
        for h in range(2):
            if k > 0:
                for way, dest, ok, prev, nbr in ((0, z + k, z + k <= nz - 1, down, up_nbr),
                                                 (1, z - k, z - k >= 0, up, down_nbr)):
                    at = jnp.clip(dest, 0, nz - 1)

                    @pl.when(ok)
                    def _():
                        landed(r1.at[c, h, at], rs1_r.at[c, h, at])

                        @pl.when(prev)
                        def _():
                            landed(r2.at[c, h, way, at], rs2_r.at[c, h, way, at])
                            add(c, h, at, (r1.at[c, h, at], r2.at[c, h, way, at]))

                        @pl.when(jnp.logical_not(prev))
                        def _():
                            add(c, h, at, (r1.at[c, h, at],))

                    send(group(y_buf, c, h, at, ycols), r2.at[c, h, way, at], rs2_s.at[c, h, way, at],
                         rs2_r.at[c, h, way, at], nbr, ok)
            else:
                landed(r1.at[c, h, z], rs1_r.at[c, h, z])
                add(c, h, z, (r1.at[c, h, z],))
                for way, prev in ((0, down), (1, up)):
                    @pl.when(prev)
                    def _():
                        landed(r2.at[c, h, way, z], rs2_r.at[c, h, way, z])
                        add(c, h, z, (r2.at[c, h, way, z],))
                mate = (y_buf.at[c, z, y, 1 - x, :, ycols[0]], y_buf.at[c, z, 1 - y, x, :, ycols[1]])[h]
                send(mate, r3.at[c, h], rs3_s.at[c, h], rs3_r.at[c, h], first_nbr[h])

    def rs_end(c):
        for h in range(2):
            landed(r3.at[c, h], rs3_r.at[c, h])
            total = y_buf[c, z, y, x, :, ycols[h]].astype(jnp.float32) + r3[c, h].astype(jnp.float32)
            out[c * ROWS:(c + 1) * ROWS, ycols[h]] = total.astype(jnp.bfloat16)

    tasks = []
    step, lag, mm = cfg["step"], cfg["lag"], cfg["mm"]
    for c in range(chunks):
        tasks.append((-1.0 + c * 0.01, functools.partial(ag_first, c)))
        t = c * lag
        for d in range(nz):
            tasks.append((t, functools.partial(ag_step, c, d)))
            t += step
        tasks.append((t, functools.partial(ag_end, c)))
        tasks.append((t + 0.01, functools.partial(ffn_in, c)))
        t += mm
        for part in range(2):
            tasks.append((t + 0.01, functools.partial(ffn_out, c, part, 2)))
            tasks.append((t + 0.02, functools.partial(rs_first, c, part)))
            t += mm / 4
        t += step
        for s in range(nz):
            tasks.append((t, functools.partial(rs_step, c, s)))
            t += step
        tasks.append((t, functools.partial(rs_end, c)))
    for _, task in sorted(tasks, key=lambda item: item[0]):
        task()

    for cp, ok in sends:
        if ok is None:
            cp.wait_send()
        else:
            pl.when(ok)(cp.wait_send)


CFG = {"step": 3.0, "lag": 7.0, "mm": 3.0}


def solution(mesh):
    n = mesh.shape["ep"]
    nz = n // 4

    def shards(tokens, expert_ids, gate_probs, w_gate, w_up, w_down):
        toks, width = tokens.shape
        ff = w_gate.shape[2]
        chunks = toks // ROWS
        half = width // 2
        bf = jnp.bfloat16
        dma = pltpu.SemaphoreType.DMA
        hbm = pl.BlockSpec(memory_space=pl.ANY)
        vmem = pl.BlockSpec(memory_space=pltpu.VMEM)
        return pl.pallas_call(
            functools.partial(kernel, n, CFG),
            out_shape=jax.ShapeDtypeStruct((toks, width), bf),
            in_specs=[hbm, vmem, vmem, hbm, hbm, hbm],
            out_specs=vmem,
            scratch_shapes=[
                pltpu.VMEM((chunks, nz, 2, 2, ROWS, width + LANES), bf),
                pltpu.VMEM((chunks, nz, 2, 2, ROWS, width), bf),
                pltpu.VMEM((chunks, 2, nz, 2, ROWS, half), bf),
                pltpu.VMEM((chunks, 2, 2, nz, 2, ROWS, half), bf),
                pltpu.VMEM((chunks, 2, ROWS, half), bf),
                pltpu.VMEM((toks, LANES), bf),
                pltpu.VMEM((n * ROWS, ff), bf),
                pltpu.VMEM((width, ff), bf),
                pltpu.VMEM((width, ff), bf),
                pltpu.VMEM((ff, width), bf),
                dma((chunks, 2)), dma((chunks, 2)),
                dma((chunks, 2, 2, nz)), dma((chunks, 2, nz)),
                dma((chunks, 2, nz)), dma((chunks, 2, nz)),
                dma((chunks, 2, nz)), dma((chunks, 2, nz)),
                dma((chunks, 2, 2, nz)), dma((chunks, 2, 2, nz)),
                dma((chunks, 2)), dma((chunks, 2)),
                dma((2 * chunks + 3,)),
            ],
            compiler_params=pltpu.CompilerParams(
                collective_id=0, has_side_effects=True, vmem_limit_bytes=60 * 1024 * 1024),
        )(tokens, expert_ids, gate_probs, w_gate, w_up, w_down)

    placed = (
        P(("dp", "ep"), None),
        P(("dp", "ep"), None),
        P(("dp", "ep"), None),
        P("ep", None, None),
        P("ep", None, None),
        P("ep", None, None),
    )
    return jax.shard_map(
        shards, mesh=mesh, in_specs=placed, out_specs=P(("dp", "ep"), None), check_vma=False
    )
```

```python
import functools

import jax
import jax.numpy as jnp
from jax import lax
from jax.experimental import pallas as pl
from jax.experimental.pallas import tpu as pltpu
from jax.sharding import PartitionSpec as P

LANES = 128
ROWS = 16
TILE = 256


def kernel(n, cfg, tokens, ids, probs, wg_hbm, wu_hbm, wd_hbm, out,
           x_buf, y_buf, r1, r2, r3, gates, hidden, wg, wu, wd,
           ag1_s, ag1_r, agz_s, agz_r, ag3_s, ag3_r,
           rs1_s, rs1_r, rs2_s, rs2_r, rs3_s, rs3_r, loc):
    nz = n // 4
    toks, width = out.shape
    chunks = toks // ROWS
    half = width // 2
    ff = wg.shape[1]
    ag_z = [c for c in range(chunks) if c % cfg["ag_every"] == cfg["ag_at"]]
    rs_z = [c for c in range(chunks) if c % cfg["rs_every"] == cfg["rs_at"]]
    me = lax.axis_index("ep")
    x, y, z = me % 2, (me // 2) % 2, me // 4
    up, down = z < nz - 1, z > 0
    dev = lambda zz, yy, xx: {"ep": (zz * 2 + yy) * 2 + xx}
    x_nbr, y_nbr = dev(z, y, 1 - x), dev(z, 1 - y, x)
    up_nbr, down_nbr = dev(jnp.minimum(z + 1, nz - 1), y, x), dev(jnp.maximum(z - 1, 0), y, x)

    wcopies = [pltpu.make_async_copy(a, b, loc.at[chunks + i])
               for i, (a, b) in enumerate(((wg_hbm.at[0], wg), (wu_hbm.at[0], wu), (wd_hbm.at[0], wd)))]
    own = []
    for c in range(chunks):
        cp = pltpu.make_async_copy(tokens.at[c * ROWS:(c + 1) * ROWS],
                                   x_buf.at[c, z, y, x, :, 0:width], loc.at[c])
        cp.start()
        own.append(cp)

    barrier = pltpu.get_barrier_semaphore()
    for nbr in (x_nbr, y_nbr):
        pl.semaphore_signal(barrier, inc=1, device_id=nbr, device_id_type=pl.DeviceIdType.MESH)
    for ok, nbr in ((up, up_nbr), (down, down_nbr)):
        @pl.when(ok)
        def _(nbr=nbr):
            pl.semaphore_signal(barrier, inc=1, device_id=nbr, device_id_type=pl.DeviceIdType.MESH)

    p = probs[...]
    w = p / jnp.sum(p, axis=0, keepdims=True)
    row = lax.broadcasted_iota(jnp.int32, (LANES, toks), 0)
    named = jnp.where(row < n, row, row - n)
    g = jnp.zeros((LANES, toks), jnp.float32)
    for k in range(ids.shape[0]):
        g = g + jnp.where(ids[k:k + 1, :] == named, w[k:k + 1, :], 0.0)
    hi = g.astype(jnp.bfloat16).astype(jnp.float32)
    gates[...] = jnp.transpose(jnp.where(row < n, hi, g - hi)).astype(jnp.bfloat16)
    gcopies = []
    for c in range(chunks):
        cp = pltpu.make_async_copy(gates.at[c * ROWS:(c + 1) * ROWS],
                                   x_buf.at[c, z, y, x, :, width:width + LANES], loc.at[chunks + 3 + c])
        cp.start()
        gcopies.append(cp)

    pl.semaphore_wait(barrier, 2 + up.astype(jnp.int32) + down.astype(jnp.int32))

    sends = []

    def send(src, dst, ssem, rsem, nbr, ok=None):
        cp = pltpu.make_async_remote_copy(src_ref=src, dst_ref=dst, send_sem=ssem, recv_sem=rsem,
                                          device_id=nbr, device_id_type=pl.DeviceIdType.MESH)
        if ok is None:
            cp.start()
        else:
            pl.when(ok)(cp.start)
        sends.append((cp, ok))

    def landed(dst, rsem):
        pltpu.make_async_copy(dst, dst, rsem).wait()

    cols = (slice(0, half), slice(half, width + LANES))
    ycols = (slice(0, half), slice(half, width))
    first_nbr, last_nbr = (x_nbr, y_nbr), (y_nbr, x_nbr)

    def group(buf, c, h, zz, cs, other=False):
        if h == 0:
            return buf.at[c, zz, (1 - y) if other else y, :, :, cs[0]]
        return buf.at[c, zz, :, (1 - x) if other else x, :, cs[1]]

    def mate(buf, c, h, zz, cs):
        return buf.at[c, zz, y, 1 - x, :, cs[0]] if h == 0 else buf.at[c, zz, 1 - y, x, :, cs[1]]

    def mine(buf, c, h, zz, cs):
        return buf.at[c, zz, y, x, :, cs[h]]

    def ag_first(c):
        own[c].wait()
        gcopies[c].wait()
        if c not in ag_z:
            for h in range(2):
                ag_pair(c, h, z)

    def ag_pair(c, h, zz, ok=None):
        blk = mine(x_buf, c, h, zz, cols)
        send(blk, blk, ag1_s.at[c, h, zz], ag1_r.at[c, h, zz], first_nbr[h], ok)

    def ag_last(c, h, zz, ok=None):
        blk = group(x_buf, c, h, zz, cols)
        send(blk, blk, ag3_s.at[c, h, zz], ag3_r.at[c, h, zz], last_nbr[h], ok)

    def ag_step(c, d):
        part = mine if c in ag_z else group
        spread = ag_pair if c in ag_z else ag_last
        for h in range(2):
            if d == 0:
                if c not in ag_z:
                    landed(mate(x_buf, c, h, z, cols), ag1_r.at[c, h, z])
                blk = part(x_buf, c, h, z, cols)
                send(blk, blk, agz_s.at[c, h, 0, z], agz_r.at[c, h, z], up_nbr, up)
                send(blk, blk, agz_s.at[c, h, 1, z], agz_r.at[c, h, z], down_nbr, down)
                spread(c, h, z)
            else:
                for way, origin, ok, more, nbr in ((0, z - d, z - d >= 0, up, up_nbr),
                                                   (1, z + d, z + d <= nz - 1, down, down_nbr)):
                    at = jnp.clip(origin, 0, nz - 1)
                    blk = part(x_buf, c, h, at, cols)
                    pl.when(ok)(functools.partial(landed, blk, agz_r.at[c, h, at]))
                    if d < nz - 1:
                        send(blk, blk, agz_s.at[c, h, way, at], agz_r.at[c, h, at], nbr, jnp.logical_and(ok, more))
                    spread(c, h, at, ok)

    def ag_mid(c, d):
        for h in range(2):
            for origin, ok in ((z - d, z - d >= 0), (z + d, z + d <= nz - 1))[:2 if d else 1]:
                at = jnp.clip(origin, 0, nz - 1)
                pl.when(ok)(functools.partial(landed, mate(x_buf, c, h, at, cols), ag1_r.at[c, h, at]))
                ag_last(c, h, at, ok)

    def ag_end(c):
        for h in range(2):
            for zz in range(nz):
                landed(group(x_buf, c, h, zz, cols, True), ag3_r.at[c, h, zz])

    rows = n * ROWS

    def ffn_in(c):
        if c == 0:
            wcopies[0].wait()
            wcopies[1].wait()
        tail = x_buf[c, :, :, :, :, width:width + LANES].reshape(rows, LANES).astype(jnp.float32)
        lanes = lax.broadcasted_iota(jnp.int32, (rows, LANES), 1)
        mine = jnp.logical_or(lanes == me, lanes == me + n)
        gcol = jnp.sum(jnp.where(mine, tail, 0.0), axis=1, keepdims=True)

        def body(j, carry):
            at = pl.ds(pl.multiple_of(j * TILE, TILE), TILE)
            xs = x_buf[c, :, :, :, :, 0:width].reshape(rows, width)
            ga = jnp.dot(xs, wg[:, at], preferred_element_type=jnp.float32)
            ua = jnp.dot(xs, wu[:, at], preferred_element_type=jnp.float32)
            hidden[:, at] = (ga / (1.0 + jnp.exp(-ga)) * ua * gcol).astype(jnp.bfloat16)
            return carry

        lax.fori_loop(0, ff // TILE, body, 0)

    def ffn_out(c, part, parts):
        if c == 0 and part == 0:
            wcopies[2].wait()
        per = width // TILE // parts

        def body(j, carry):
            at = pl.ds(pl.multiple_of(j * TILE, TILE), TILE)
            o = jnp.dot(hidden[...], wd[:, at], preferred_element_type=jnp.float32)
            y_buf[c, :, :, :, :, at] = o.astype(jnp.bfloat16).reshape(nz, 2, 2, ROWS, TILE)
            return carry

        lax.fori_loop(part * per, (part + 1) * per, body, 0)

    def rs_first(c, h):
        for i in range(nz):
            zz = jnp.where(z >= nz // 2, i, nz - 1 - i)
            send(group(y_buf, c, h, zz, ycols, True), r1.at[c, h, zz], rs1_s.at[c, h, zz],
                 rs1_r.at[c, h, zz], last_nbr[h])

    def add(place, bufs):
        total = place[...].astype(jnp.float32)
        for b in bufs:
            total = total + b[...].astype(jnp.float32)
        place[...] = total.astype(jnp.bfloat16)

    def rs_mid(c, s):
        k = nz - 1 - s
        for h in range(2):
            for dest, ok in ((z + k, z + k <= nz - 1), (z - k, z - k >= 0))[:2 if k else 1]:
                at = jnp.clip(dest, 0, nz - 1)

                @pl.when(ok)
                def _():
                    landed(r1.at[c, h, at], rs1_r.at[c, h, at])
                    add(group(y_buf, c, h, at, ycols), (r1.at[c, h, at],))

                send(mate(y_buf, c, h, at, ycols), r3.at[c, h, at], rs3_s.at[c, h, at],
                     rs3_r.at[c, h, at], first_nbr[h], ok)

    def rs_step(c, s):
        k = nz - 1 - s
        part = mine if c in rs_z else group
        before = (r3, rs3_r) if c in rs_z else (r1, rs1_r)
        hop = lambda h, way, at: r2.at[c, h, way, at, 0] if c in rs_z else r2.at[c, h, way, at]
        for h in range(2):
            if k > 0:
                for way, dest, ok, prev, nbr in ((0, z + k, z + k <= nz - 1, down, up_nbr),
                                                 (1, z - k, z - k >= 0, up, down_nbr)):
                    at = jnp.clip(dest, 0, nz - 1)
                    place, buf = part(y_buf, c, h, at, ycols), before[0].at[c, h, at]

                    @pl.when(ok)
                    def _():
                        landed(buf, before[1].at[c, h, at])

                        @pl.when(prev)
                        def _():
                            landed(hop(h, way, at), rs2_r.at[c, h, way, at])
                            add(place, (buf, hop(h, way, at)))

                        @pl.when(jnp.logical_not(prev))
                        def _():
                            add(place, (buf,))

                    send(place, hop(h, way, at), rs2_s.at[c, h, way, at],
                         rs2_r.at[c, h, way, at], nbr, ok)
            else:
                place = part(y_buf, c, h, z, ycols)
                landed(before[0].at[c, h, z], before[1].at[c, h, z])
                add(place, (before[0].at[c, h, z],))
                for way, prev in ((0, down), (1, up)):
                    @pl.when(prev)
                    def _():
                        landed(hop(h, way, z), rs2_r.at[c, h, way, z])
                        add(place, (hop(h, way, z),))
                if c in rs_z:
                    out[c * ROWS:(c + 1) * ROWS, ycols[h]] = place[...]
                else:
                    send(mate(y_buf, c, h, z, ycols), r3.at[c, h, z], rs3_s.at[c, h, z],
                         rs3_r.at[c, h, z], first_nbr[h])

    def rs_end(c):
        for h in range(2):
            landed(r3.at[c, h, z], rs3_r.at[c, h, z])
            total = mine(y_buf, c, h, z, ycols)[...].astype(jnp.float32) + r3[c, h, z].astype(jnp.float32)
            out[c * ROWS:(c + 1) * ROWS, ycols[h]] = total.astype(jnp.bfloat16)

    def weights():
        for cp in wcopies:
            cp.start()

    tasks = [(-8.995, weights)]
    step, lag, mm, rlag = cfg["step"], cfg["lag"], cfg["mm"], cfg["rlag"]
    for c in range(chunks):
        tasks.append((-9.0 + c * 0.01, functools.partial(ag_first, c)))
        t = c * lag
        for d in range(nz):
            if c in ag_z:
                tasks.append((t - step, functools.partial(ag_step, c, d)))
                tasks.append((t, functools.partial(ag_mid, c, d)))
            else:
                tasks.append((t, functools.partial(ag_step, c, d)))
            t += step
        tasks.append((t, functools.partial(ag_end, c)))
        tasks.append((t + 0.01, functools.partial(ffn_in, c)))
        t += mm
        for part in range(2):
            tasks.append((t + 0.01, functools.partial(ffn_out, c, part, 2)))
            tasks.append((t + 0.02, functools.partial(rs_first, c, part)))
            t += mm / 4
        t += cfg["wait"] + c * (rlag - lag)
        for s in range(nz):
            if c in rs_z:
                tasks.append((t, functools.partial(rs_mid, c, s)))
                tasks.append((t + step, functools.partial(rs_step, c, s)))
            else:
                tasks.append((t, functools.partial(rs_step, c, s)))
            t += step
        if c not in rs_z:
            tasks.append((t, functools.partial(rs_end, c)))
    for _, task in sorted(tasks, key=lambda item: item[0]):
        task()

    for cp, ok in sends:
        if ok is None:
            cp.wait_send()
        else:
            pl.when(ok)(cp.wait_send)


CFG = {"step": 3.0, "lag": 5.0, "mm": 3.0, "rlag": 5.0, "wait": 3.0, "ag_every": 4, "ag_at": 0, "rs_every": 4, "rs_at": 3}


def solution(mesh):
    n = mesh.shape["ep"]
    nz = n // 4

    def shards(tokens, expert_ids, gate_probs, w_gate, w_up, w_down):
        toks, width = tokens.shape
        ff = w_gate.shape[2]
        chunks = toks // ROWS
        half = width // 2
        bf = jnp.bfloat16
        dma = pltpu.SemaphoreType.DMA
        hbm = pl.BlockSpec(memory_space=pl.ANY)
        vmem = pl.BlockSpec(memory_space=pltpu.VMEM)
        return pl.pallas_call(
            functools.partial(kernel, n, CFG),
            out_shape=jax.ShapeDtypeStruct((toks, width), bf),
            in_specs=[hbm, vmem, vmem, hbm, hbm, hbm],
            out_specs=vmem,
            scratch_shapes=[
                pltpu.VMEM((chunks, nz, 2, 2, ROWS, width + LANES), bf),
                pltpu.VMEM((chunks, nz, 2, 2, ROWS, width), bf),
                pltpu.VMEM((chunks, 2, nz, 2, ROWS, half), bf),
                pltpu.VMEM((chunks, 2, 2, nz, 2, ROWS, half), bf),
                pltpu.VMEM((chunks, 2, nz, ROWS, half), bf),
                pltpu.VMEM((toks, LANES), bf),
                pltpu.VMEM((n * ROWS, ff), bf),
                pltpu.VMEM((width, ff), bf),
                pltpu.VMEM((width, ff), bf),
                pltpu.VMEM((ff, width), bf),
                dma((chunks, 2, nz)), dma((chunks, 2, nz)),
                dma((chunks, 2, 2, nz)), dma((chunks, 2, nz)),
                dma((chunks, 2, nz)), dma((chunks, 2, nz)),
                dma((chunks, 2, nz)), dma((chunks, 2, nz)),
                dma((chunks, 2, 2, nz)), dma((chunks, 2, 2, nz)),
                dma((chunks, 2, nz)), dma((chunks, 2, nz)),
                dma((2 * chunks + 3,)),
            ],
            compiler_params=pltpu.CompilerParams(
                collective_id=0, has_side_effects=True, vmem_limit_bytes=60 * 1024 * 1024),
        )(tokens, expert_ids.T, gate_probs.T, w_gate, w_up, w_down)

    placed = (
        P(("dp", "ep"), None),
        P(("dp", "ep"), None),
        P(("dp", "ep"), None),
        P("ep", None, None),
        P("ep", None, None),
        P("ep", None, None),
    )
    return jax.shard_map(
        shards, mesh=mesh, in_specs=placed, out_specs=P(("dp", "ep"), None), check_vma=False
    )
```

```python
import functools

import jax
import jax.numpy as jnp
from jax import lax
from jax.experimental import pallas as pl
from jax.experimental.pallas import tpu as pltpu
from jax.sharding import PartitionSpec as P

LANES = 128
ROWS = 16
TILE = 256


def kernel(n, cfg, tokens, ids, probs, wg_hbm, wu_hbm, wd_hbm, out,
           x_buf, y_buf, r1, r2, r3, gates, hidden, wg, wu, wd,
           ag1_s, ag1_r, agz_s, agz_r, ag3_s, ag3_r,
           rs1_s, rs1_r, rs2_s, rs2_r, rs3_s, rs3_r, loc):
    nz = n // 4
    toks, width = out.shape
    chunks = toks // ROWS
    half = width // 2
    ff = wg.shape[1]
    ag_z = [c for c in range(chunks) if c % cfg["ag_every"] == cfg["ag_at"]]
    rs_z = [c for c in range(chunks) if c % cfg["rs_every"] == cfg["rs_at"]]
    me = lax.axis_index("ep")
    x, y, z = me % 2, (me // 2) % 2, me // 4
    up, down = z < nz - 1, z > 0
    dev = lambda zz, yy, xx: {"ep": (zz * 2 + yy) * 2 + xx}
    x_nbr, y_nbr = dev(z, y, 1 - x), dev(z, 1 - y, x)
    up_nbr, down_nbr = dev(jnp.minimum(z + 1, nz - 1), y, x), dev(jnp.maximum(z - 1, 0), y, x)

    wcopies = [pltpu.make_async_copy(a, b, loc.at[chunks + i])
               for i, (a, b) in enumerate(((wg_hbm.at[0], wg), (wu_hbm.at[0], wu), (wd_hbm.at[0], wd)))]
    own = []
    for c in range(chunks):
        cp = pltpu.make_async_copy(tokens.at[c * ROWS:(c + 1) * ROWS],
                                   x_buf.at[c, z, y, x, :, 0:width], loc.at[c])
        cp.start()
        own.append(cp)

    barrier = pltpu.get_barrier_semaphore()
    for nbr in (x_nbr, y_nbr):
        pl.semaphore_signal(barrier, inc=1, device_id=nbr, device_id_type=pl.DeviceIdType.MESH)
    for ok, nbr in ((up, up_nbr), (down, down_nbr)):
        @pl.when(ok)
        def _(nbr=nbr):
            pl.semaphore_signal(barrier, inc=1, device_id=nbr, device_id_type=pl.DeviceIdType.MESH)

    p = probs[...]
    w = p / jnp.sum(p, axis=0, keepdims=True)
    row = lax.broadcasted_iota(jnp.int32, (LANES, toks), 0)
    named = jnp.where(row < n, row, row - n)
    g = jnp.zeros((LANES, toks), jnp.float32)
    for k in range(ids.shape[0]):
        g = g + jnp.where(ids[k:k + 1, :] == named, w[k:k + 1, :], 0.0)
    hi = g.astype(jnp.bfloat16).astype(jnp.float32)
    gates[...] = jnp.transpose(jnp.where(row < n, hi, g - hi)).astype(jnp.bfloat16)
    gcopies = []
    for c in range(chunks):
        cp = pltpu.make_async_copy(gates.at[c * ROWS:(c + 1) * ROWS],
                                   x_buf.at[c, z, y, x, :, width:width + LANES], loc.at[chunks + 3 + c])
        cp.start()
        gcopies.append(cp)

    pl.semaphore_wait(barrier, 2 + up.astype(jnp.int32) + down.astype(jnp.int32))

    sends = []

    def send(src, dst, ssem, rsem, nbr, ok=None):
        cp = pltpu.make_async_remote_copy(src_ref=src, dst_ref=dst, send_sem=ssem, recv_sem=rsem,
                                          device_id=nbr, device_id_type=pl.DeviceIdType.MESH)
        if ok is None:
            cp.start()
        else:
            pl.when(ok)(cp.start)
        sends.append((cp, ok))

    def landed(dst, rsem):
        pltpu.make_async_copy(dst, dst, rsem).wait()

    cols = (slice(0, half), slice(half, width + LANES))
    ycols = (slice(0, half), slice(half, width))
    first_nbr, last_nbr = (x_nbr, y_nbr), (y_nbr, x_nbr)

    def group(buf, c, h, zz, cs, other=False):
        if h == 0:
            return buf.at[c, zz, (1 - y) if other else y, :, :, cs[0]]
        return buf.at[c, zz, :, (1 - x) if other else x, :, cs[1]]

    def mate(buf, c, h, zz, cs):
        return buf.at[c, zz, y, 1 - x, :, cs[0]] if h == 0 else buf.at[c, zz, 1 - y, x, :, cs[1]]

    def mine(buf, c, h, zz, cs):
        return buf.at[c, zz, y, x, :, cs[h]]

    def ag_first(c):
        own[c].wait()
        gcopies[c].wait()
        if c not in ag_z:
            for h in range(2):
                ag_pair(c, h, z)

    def ag_pair(c, h, zz, ok=None):
        blk = mine(x_buf, c, h, zz, cols)
        send(blk, blk, ag1_s.at[c, h, zz], ag1_r.at[c, h, zz], first_nbr[h], ok)

    def ag_last(c, h, zz, ok=None):
        blk = group(x_buf, c, h, zz, cols)
        send(blk, blk, ag3_s.at[c, h, zz], ag3_r.at[c, h, zz], last_nbr[h], ok)

    def ag_step(c, d):
        part = mine if c in ag_z else group
        spread = ag_pair if c in ag_z else ag_last
        for h in range(2):
            if d == 0:
                if c not in ag_z:
                    landed(mate(x_buf, c, h, z, cols), ag1_r.at[c, h, z])
                blk = part(x_buf, c, h, z, cols)
                send(blk, blk, agz_s.at[c, h, 0, z], agz_r.at[c, h, z], up_nbr, up)
                send(blk, blk, agz_s.at[c, h, 1, z], agz_r.at[c, h, z], down_nbr, down)
                spread(c, h, z)
            else:
                for way, origin, ok, more, nbr in ((0, z - d, z - d >= 0, up, up_nbr),
                                                   (1, z + d, z + d <= nz - 1, down, down_nbr)):
                    at = jnp.clip(origin, 0, nz - 1)
                    blk = part(x_buf, c, h, at, cols)
                    pl.when(ok)(functools.partial(landed, blk, agz_r.at[c, h, at]))
                    if d < nz - 1:
                        send(blk, blk, agz_s.at[c, h, way, at], agz_r.at[c, h, at], nbr, jnp.logical_and(ok, more))
                    spread(c, h, at, ok)

    def ag_mid(c, d):
        for h in range(2):
            for origin, ok in ((z - d, z - d >= 0), (z + d, z + d <= nz - 1))[:2 if d else 1]:
                at = jnp.clip(origin, 0, nz - 1)
                pl.when(ok)(functools.partial(landed, mate(x_buf, c, h, at, cols), ag1_r.at[c, h, at]))
                ag_last(c, h, at, ok)

    def ag_end(c):
        for h in range(2):
            for zz in range(nz):
                landed(group(x_buf, c, h, zz, cols, True), ag3_r.at[c, h, zz])

    rows = n * ROWS

    def ffn_in(c):
        if c == 0:
            wcopies[0].wait()
            wcopies[1].wait()
        tail = x_buf[c, :, :, :, :, width:width + LANES].reshape(rows, LANES).astype(jnp.float32)
        lanes = lax.broadcasted_iota(jnp.int32, (rows, LANES), 1)
        mine = jnp.logical_or(lanes == me, lanes == me + n)
        gcol = jnp.sum(jnp.where(mine, tail, 0.0), axis=1, keepdims=True)

        def body(j, carry):
            at = pl.ds(pl.multiple_of(j * TILE, TILE), TILE)
            xs = x_buf[c, :, :, :, :, 0:width].reshape(rows, width)
            ga = jnp.dot(xs, wg[:, at], preferred_element_type=jnp.float32)
            ua = jnp.dot(xs, wu[:, at], preferred_element_type=jnp.float32)
            hidden[:, at] = (ga / (1.0 + jnp.exp(-ga)) * ua * gcol).astype(jnp.bfloat16)
            return carry

        lax.fori_loop(0, ff // TILE, body, 0)

    def ffn_out(c, part, parts):
        if c == 0 and part == 0:
            wcopies[2].wait()
        per = width // TILE // parts

        def body(j, carry):
            at = pl.ds(pl.multiple_of(j * TILE, TILE), TILE)
            o = jnp.dot(hidden[...], wd[:, at], preferred_element_type=jnp.float32)
            y_buf[c, :, :, :, :, at] = o.astype(jnp.bfloat16).reshape(nz, 2, 2, ROWS, TILE)
            return carry

        lax.fori_loop(part * per, (part + 1) * per, body, 0)

    def rs_first(c, h):
        for i in range(nz):
            zz = jnp.where(z >= nz // 2, i, nz - 1 - i)
            send(group(y_buf, c, h, zz, ycols, True), r1.at[c, h, zz], rs1_s.at[c, h, zz],
                 rs1_r.at[c, h, zz], last_nbr[h])

    def add(place, bufs):
        total = place[...].astype(jnp.float32)
        for b in bufs:
            total = total + b[...].astype(jnp.float32)
        place[...] = total.astype(jnp.bfloat16)

    def rs_mid(c, s):
        k = nz - 1 - s
        for h in range(2):
            for dest, ok in ((z + k, z + k <= nz - 1), (z - k, z - k >= 0))[:2 if k else 1]:
                at = jnp.clip(dest, 0, nz - 1)

                @pl.when(ok)
                def _():
                    landed(r1.at[c, h, at], rs1_r.at[c, h, at])
                    add(group(y_buf, c, h, at, ycols), (r1.at[c, h, at],))

                send(mate(y_buf, c, h, at, ycols), r3.at[c, h, at], rs3_s.at[c, h, at],
                     rs3_r.at[c, h, at], first_nbr[h], ok)

    def rs_step(c, s):
        k = nz - 1 - s
        part = mine if c in rs_z else group
        before = (r3, rs3_r) if c in rs_z else (r1, rs1_r)
        hop = lambda h, way, at: r2.at[c, h, way, at, 0] if c in rs_z else r2.at[c, h, way, at]
        for h in range(2):
            if k > 0:
                for way, dest, ok, prev, nbr in ((0, z + k, z + k <= nz - 1, down, up_nbr),
                                                 (1, z - k, z - k >= 0, up, down_nbr)):
                    at = jnp.clip(dest, 0, nz - 1)
                    place, buf = part(y_buf, c, h, at, ycols), before[0].at[c, h, at]

                    @pl.when(ok)
                    def _():
                        landed(buf, before[1].at[c, h, at])

                        @pl.when(prev)
                        def _():
                            landed(hop(h, way, at), rs2_r.at[c, h, way, at])
                            add(place, (buf, hop(h, way, at)))

                        @pl.when(jnp.logical_not(prev))
                        def _():
                            add(place, (buf,))

                    send(place, hop(h, way, at), rs2_s.at[c, h, way, at],
                         rs2_r.at[c, h, way, at], nbr, ok)
            else:
                place = part(y_buf, c, h, z, ycols)
                landed(before[0].at[c, h, z], before[1].at[c, h, z])
                add(place, (before[0].at[c, h, z],))
                for way, prev in ((0, down), (1, up)):
                    @pl.when(prev)
                    def _():
                        landed(hop(h, way, z), rs2_r.at[c, h, way, z])
                        add(place, (hop(h, way, z),))
                if c in rs_z:
                    out[c * ROWS:(c + 1) * ROWS, ycols[h]] = place[...]
                else:
                    send(mate(y_buf, c, h, z, ycols), r3.at[c, h, z], rs3_s.at[c, h, z],
                         rs3_r.at[c, h, z], first_nbr[h])

    def rs_end(c):
        for h in range(2):
            landed(r3.at[c, h, z], rs3_r.at[c, h, z])
            total = mine(y_buf, c, h, z, ycols)[...].astype(jnp.float32) + r3[c, h, z].astype(jnp.float32)
            out[c * ROWS:(c + 1) * ROWS, ycols[h]] = total.astype(jnp.bfloat16)

    def weights():
        for cp in wcopies:
            cp.start()

    tasks = [(-8.995, weights)]
    step, lag, mm, rlag = cfg["step"], cfg["lag"], cfg["mm"], cfg["rlag"]
    for c in range(chunks):
        tasks.append((-9.0 + c * 0.01, functools.partial(ag_first, c)))
        t = c * lag
        for d in range(nz):
            if c in ag_z:
                tasks.append((t - step, functools.partial(ag_step, c, d)))
                tasks.append((t, functools.partial(ag_mid, c, d)))
            else:
                tasks.append((t, functools.partial(ag_step, c, d)))
            t += step
        tasks.append((t, functools.partial(ag_end, c)))
        tasks.append((t + 0.01, functools.partial(ffn_in, c)))
        t += mm
        for part in range(2):
            tasks.append((t + 0.01, functools.partial(ffn_out, c, part, 2)))
            tasks.append((t + 0.02, functools.partial(rs_first, c, part)))
            t += mm / 4
        t += cfg["wait"] + c * (rlag - lag)
        for s in range(nz):
            if c in rs_z:
                tasks.append((t, functools.partial(rs_mid, c, s)))
                tasks.append((t + step, functools.partial(rs_step, c, s)))
            else:
                tasks.append((t, functools.partial(rs_step, c, s)))
            t += step
        if c not in rs_z:
            tasks.append((t, functools.partial(rs_end, c)))
    for _, task in sorted(tasks, key=lambda item: item[0]):
        task()

    for cp, ok in sends:
        if ok is None:
            cp.wait_send()
        else:
            pl.when(ok)(cp.wait_send)


CFG = {"step": 3.0, "lag": 5.0, "mm": 3.0, "rlag": 4.0, "wait": 3.0, "ag_every": 4, "ag_at": 0, "rs_every": 4, "rs_at": 3}


def solution(mesh):
    n = mesh.shape["ep"]
    nz = n // 4

    def shards(tokens, expert_ids, gate_probs, w_gate, w_up, w_down):
        toks, width = tokens.shape
        ff = w_gate.shape[2]
        chunks = toks // ROWS
        half = width // 2
        bf = jnp.bfloat16
        dma = pltpu.SemaphoreType.DMA
        hbm = pl.BlockSpec(memory_space=pl.ANY)
        vmem = pl.BlockSpec(memory_space=pltpu.VMEM)
        return pl.pallas_call(
            functools.partial(kernel, n, CFG),
            out_shape=jax.ShapeDtypeStruct((toks, width), bf),
            in_specs=[hbm, vmem, vmem, hbm, hbm, hbm],
            out_specs=vmem,
            scratch_shapes=[
                pltpu.VMEM((chunks, nz, 2, 2, ROWS, width + LANES), bf),
                pltpu.VMEM((chunks, nz, 2, 2, ROWS, width), bf),
                pltpu.VMEM((chunks, 2, nz, 2, ROWS, half), bf),
                pltpu.VMEM((chunks, 2, 2, nz, 2, ROWS, half), bf),
                pltpu.VMEM((chunks, 2, nz, ROWS, half), bf),
                pltpu.VMEM((toks, LANES), bf),
                pltpu.VMEM((n * ROWS, ff), bf),
                pltpu.VMEM((width, ff), bf),
                pltpu.VMEM((width, ff), bf),
                pltpu.VMEM((ff, width), bf),
                dma((chunks, 2, nz)), dma((chunks, 2, nz)),
                dma((chunks, 2, 2, nz)), dma((chunks, 2, nz)),
                dma((chunks, 2, nz)), dma((chunks, 2, nz)),
                dma((chunks, 2, nz)), dma((chunks, 2, nz)),
                dma((chunks, 2, 2, nz)), dma((chunks, 2, 2, nz)),
                dma((chunks, 2, nz)), dma((chunks, 2, nz)),
                dma((2 * chunks + 3,)),
            ],
            compiler_params=pltpu.CompilerParams(
                collective_id=0, has_side_effects=True, vmem_limit_bytes=60 * 1024 * 1024),
        )(tokens, expert_ids.T, gate_probs.T, w_gate, w_up, w_down)

    placed = (
        P(("dp", "ep"), None),
        P(("dp", "ep"), None),
        P(("dp", "ep"), None),
        P("ep", None, None),
        P("ep", None, None),
        P("ep", None, None),
    )
    return jax.shard_map(
        shards, mesh=mesh, in_specs=placed, out_specs=P(("dp", "ep"), None), check_vma=False
    )
```
